32 devices in a mesh: grp: 2 (over x), seq: 8 (over z, y), head: 2 (over core).
Axes of the slice: x: 2, y: 2, z: 4, core: 2. Of those that a mesh axis runs over, the one named last changes fastest.
Arguments:
- features: bfloat16 [2, 8, 4, 32, 512], P('grp', 'seq', 'head'), may hold values from -6 to 6
- conv_weight: bfloat16 [3, 3, 3, 512, 16], replicated, may hold values from -0.0546875 to 0.0546875
- conv_bias: float32 [16], replicated, may hold values from -3 to 3
- token_order: int32 [256], P('seq'), may hold values from 0 to 255, each once
- embed_weight: bfloat16 [64, 3072], replicated, may hold values from -0.75 to 0.75
- norm_gain: float32 [3072], replicated, may hold values from 0.1 to 1.9
- qkv_weight: bfloat16 [3072, 3, 2048], P('seq', None, 'head'), may hold values from -0.109375 to 0.109375
- grad_out: bfloat16 [2, 256, 2048], P('grp', 'seq', 'head'), may hold values from -6 to 6
Outputs:
- attended: bfloat16 [2, 256, 2048], P('grp', 'seq', 'head')
- embed_grad: float32 [64, 3072], P(None, 'head')
The draws below stay inside these ranges and needn't reach their ends.
All inputs are finite; a program needn't handle non-finite values.
Results may differ from the reference program's by a relative error of at most 0.0052.
Values may be sent and summed in bfloat16 or wider, within the bound.
A program may use at most 128 MiB of HBM per device.

```python
import jax
import jax.numpy as jnp
from jax import lax

C_ENC = 512
LAT = 16
D = 3072
HEADS = 32
HEAD_DIM = 64
LW = 32
CLIPS = 2
FRAMES = 8
LH = 4
PATCH = 64
TOKENS = 256


def levels(key, extent, split, smallest, largest):
    def one(dim, shards_of):
        draws = jax.random.uniform(jax.random.fold_in(jax.random.fold_in(key, 6), dim), (shards_of,), jnp.float32, smallest / len(split), largest / len(split))
        return jnp.repeat(jnp.exp(draws), extent[dim] // shards_of).reshape((-1,) + (1,) * (len(extent) - dim - 1))

    factor_of = one(*split[0])
    for cut in split[1:]:
        factor_of = factor_of * one(*cut)
    return factor_of


def bell_draw(own_key, shape, spread, most, split=(), kind=jnp.bfloat16):
    result = jax.random.normal(own_key, shape, jnp.float32) * spread
    if len(split) > 0:
        result = levels(own_key, shape, split, -0.22, 0.18) * result
    return jnp.clip(result, min=-most, max=most).astype(kind)


def setup_inputs(seed: int = 0) -> dict:
    splits = jax.random.split(jax.random.key(seed), 9)
    features = bell_draw(splits[0], (CLIPS, FRAMES, LH, LW, C_ENC), 1.0, 6.0, ((0, 2), (1, 8), (2, 2)))
    conv_weight = bell_draw(splits[1], (3, 3, 3, C_ENC, LAT), (27 * C_ENC) ** -0.5, 0.0546875)
    conv_bias = bell_draw(splits[2], (LAT,), 0.5, 3.0, (), jnp.float32)
    token_order = jax.random.permutation(splits[3], TOKENS).astype(jnp.int32)
    embed_weight = bell_draw(splits[4], (PATCH, D), PATCH ** -0.5, 0.75)
    norm_gain = jnp.clip(1.0 + 0.18 * jax.random.normal(splits[5], (D,), jnp.float32), 0.1, 1.9)
    qkv_weight = bell_draw(splits[6], (D, 3, HEADS * HEAD_DIM), D ** -0.5, 0.109375, ((0, 8), (2, 2)))
    grad_out = bell_draw(splits[7], (CLIPS, TOKENS, HEADS * HEAD_DIM), 1.0, 6.0, ((0, 2), (1, 8), (2, 2)))
    return dict(features=features, conv_weight=conv_weight, conv_bias=conv_bias, token_order=token_order, embed_weight=embed_weight, norm_gain=norm_gain, qkv_weight=qkv_weight, grad_out=grad_out)


def encode(clip_feat, conv_weight, conv_bias):
    padded = jnp.pad(clip_feat, ((2, 0), (1, 1), (1, 1), (0, 0)))
    total = jnp.zeros((FRAMES * LH * LW, LAT), jnp.float32) + conv_bias
    for a in range(3):
        for b in range(3):
            for e in range(3):
                piece = padded[a:a + FRAMES, b:b + LH, e:e + LW].reshape(-1, C_ENC)
                total = total + jnp.dot(piece, conv_weight[a, b, e], preferred_element_type=jnp.float32)
    return total.astype(jnp.bfloat16).reshape(FRAMES, LH, LW, LAT)

def patchify(latent):
    frames = latent.shape[0]
    blocks = latent.reshape(frames, LH // 2, 2, LW // 2, 2, LAT)
    blocks = jnp.transpose(blocks, (0, 1, 3, 2, 4, 5))
    return blocks.reshape(frames * (LH // 2) * (LW // 2), 4 * LAT)

def one_head(operands):
    query, keys, values, cotan = operands
    factor = HEAD_DIM ** (-0.5)
    scores = jnp.dot(query, keys.T, preferred_element_type=jnp.float32) * factor
    top = lax.optimization_barrier(jnp.max(scores, axis=-1, keepdims=True))
    lse = top + jnp.log(lax.optimization_barrier(jnp.sum(jnp.exp(scores - top), axis=-1, keepdims=True)))
    probs = jnp.exp(scores - lse)
    probs_low = probs.astype(jnp.bfloat16)
    output = jnp.dot(probs_low, values, preferred_element_type=jnp.float32).astype(jnp.bfloat16)
    delta = lax.optimization_barrier(jnp.sum(cotan.astype(jnp.float32) * output.astype(jnp.float32), axis=-1, keepdims=True))
    dprob = jnp.dot(cotan, values.T, preferred_element_type=jnp.float32)
    dscore = (probs * (dprob - delta)).astype(jnp.bfloat16)
    grad_q = jnp.dot(dscore, keys, preferred_element_type=jnp.float32) * factor
    grad_k = jnp.dot(dscore.T, query, preferred_element_type=jnp.float32) * factor
    grad_v = jnp.dot(probs_low.T, cotan, preferred_element_type=jnp.float32)
    return (output, grad_q, grad_k, grad_v)

def per_heads(matrix):
    return jnp.transpose(matrix.reshape(TOKENS, HEADS, HEAD_DIM), (1, 0, 2))

def from_heads(stacked):
    return jnp.transpose(stacked, (1, 0, 2)).reshape(TOKENS, HEADS * HEAD_DIM)

def reference(features, conv_weight, conv_bias, token_order, embed_weight, norm_gain, qkv_weight, grad_out):
    width = HEADS * HEAD_DIM
    flat_weight = qkv_weight.reshape(D, 3 * width)
    outputs = []
    embed_grad = jnp.zeros((PATCH, D), jnp.float32)
    for clip in range(CLIPS):
        latent = encode(features[clip], conv_weight, conv_bias)
        patches = patchify(latent)
        tokens = jnp.take(patches, token_order.astype(jnp.int32), axis=0)
        mixed = jnp.dot(tokens, embed_weight, preferred_element_type=jnp.float32)
        inverse = lax.rsqrt(lax.optimization_barrier(jnp.mean(mixed * mixed, axis=-1, keepdims=True)) + 1e-06)
        normal = mixed * inverse
        hidden = (normal * norm_gain).astype(jnp.bfloat16)
        proj = jnp.dot(hidden, flat_weight, preferred_element_type=jnp.float32).astype(jnp.bfloat16)
        proj = proj.reshape(TOKENS, 3, width)
        output, grad_q, grad_k, grad_v = lax.map(one_head, (per_heads(proj[:, 0]), per_heads(proj[:, 1]), per_heads(proj[:, 2]), per_heads(grad_out[clip])))
        outputs.append(from_heads(output))
        grads = jnp.stack([from_heads(grad_q), from_heads(grad_k), from_heads(grad_v)], axis=1).reshape(TOKENS, 3 * width).astype(jnp.bfloat16)
        back = jnp.dot(grads, flat_weight.T, preferred_element_type=jnp.float32)
        scaled = back * norm_gain
        inner = lax.optimization_barrier(jnp.mean(scaled * normal, axis=-1, keepdims=True))
        dmixed = inverse * (scaled - normal * inner)
        embed_grad = embed_grad + jnp.dot(tokens.astype(jnp.float32).T, dmixed, preferred_element_type=jnp.float32, precision=lax.Precision.HIGHEST)
    return (jnp.stack(outputs, axis=0), embed_grad)
```

```python
import functools

import jax
import jax.numpy as jnp
from jax import lax
from jax.experimental import pallas as pl
from jax.experimental.pallas import tpu as pltpu
from jax.sharding import PartitionSpec as P

D = 3072
HEAD_DIM = 64
MESH = pl.DeviceIdType.MESH


def shifted(value, axis, steps):
    count = lax.axis_size(axis)
    leading, last = (max(0, -steps), min(count, count - steps))
    return lax.ppermute(value, axis, [(source, source + steps) for source in range(leading, last)])


def extended(block, sides, width):
    for axis, dim in sides:
        count = lax.axis_size(axis)
        forward = [(i, i + 1) for i in range(count - 1)]
        backward = [(target, source) for source, target in forward]
        low = lax.ppermute(
            lax.slice_in_dim(block, block.shape[dim] - width, None, axis=dim), axis, forward
        )
        high = lax.ppermute(lax.slice_in_dim(block, 0, width, axis=dim), axis, backward)
        block = jnp.concatenate([low, block, high], axis=dim)
    return block


def patchify(latent):
    frames, rows, columns, channels = latent.shape
    blocks = latent.reshape(frames, rows // 2, 2, columns // 2, 2, channels)
    blocks = jnp.transpose(blocks, (0, 1, 3, 2, 4, 5))
    return blocks.reshape(frames * (rows // 2) * (columns // 2), 4 * channels)


def encode_tile(tile, conv_weight, conv_bias):
    frames, rows, columns, channels = tile.shape
    hops = (frames + 1) // frames
    earlier = []
    for hop in range(hops, 0, -1):
        earlier.append(shifted(tile, "seq", hop))
    stacked = jnp.concatenate(earlier + [tile], axis=0)
    padded = extended(stacked, (("head", 1),), 1)
    padded = jnp.pad(padded, ((0, 0), (0, 0), (1, 1), (0, 0)))
    total = jnp.zeros((frames * rows * columns, conv_weight.shape[-1]), jnp.float32) + conv_bias
    for a in range(3):
        for b in range(3):
            for e in range(3):
                piece = padded[a : a + frames, b : b + rows, e : e + columns].reshape(-1, channels)
                total = total + jnp.dot(
                    piece, conv_weight[a, b, e], preferred_element_type=jnp.float32
                )
    return total.astype(jnp.bfloat16).reshape(frames, rows, columns, conv_weight.shape[-1])


def head_major(matrix, head_local):
    count = matrix.shape[0]
    return jnp.transpose(matrix.reshape(count, head_local, HEAD_DIM), (1, 0, 2))


def row_major(stacked):
    heads_here, count, size = stacked.shape
    return jnp.transpose(stacked, (1, 0, 2)).reshape(count, heads_here * size)


def head_forward(operands):
    query, keys, values, cotan = operands
    factor = HEAD_DIM ** (-0.5)
    scores = jnp.dot(query, keys.T, preferred_element_type=jnp.float32) * factor
    top = jnp.max(scores, axis=-1, keepdims=True)
    lse = top + jnp.log(jnp.sum(jnp.exp(scores - top), axis=-1, keepdims=True))
    probs = jnp.exp(scores - lse)
    probs_low = probs.astype(jnp.bfloat16)
    output = jnp.dot(probs_low, values, preferred_element_type=jnp.float32).astype(jnp.bfloat16)
    delta = jnp.sum(cotan.astype(jnp.float32) * output.astype(jnp.float32), axis=-1, keepdims=True)
    dprob = jnp.dot(cotan, values.T, preferred_element_type=jnp.float32)
    dscore = (probs * (dprob - delta)).astype(jnp.bfloat16)
    grad_q = jnp.dot(dscore, keys, preferred_element_type=jnp.float32) * factor
    return (output, lse[:, 0], delta[:, 0], grad_q)


def head_backward(operands):
    query, cotan, lse_piece, delta_piece, own_keys, own_values = operands
    factor = HEAD_DIM ** (-0.5)
    scores = jnp.dot(query, own_keys.T, preferred_element_type=jnp.float32) * factor
    probs = jnp.exp(scores - lse_piece[:, None])
    value_add = jnp.dot(probs.astype(jnp.bfloat16).T, cotan, preferred_element_type=jnp.float32)
    dprob = jnp.dot(cotan, own_values.T, preferred_element_type=jnp.float32)
    dscore = (probs * (dprob - delta_piece[:, None])).astype(jnp.bfloat16)
    key_add = jnp.dot(dscore.T, query, preferred_element_type=jnp.float32)
    return (key_add, value_add)


def per_device(
    features, conv_weight, conv_bias, token_order, embed_weight, norm_gain, qkv_weight, grad_out
):
    tile = encode_tile(features[0], conv_weight, conv_bias)
    all_rows = lax.all_gather(tile, "head", axis=1, tiled=True)
    whole = lax.all_gather(all_rows, "seq", axis=0, tiled=True)
    patches = patchify(whole)
    tokens = jnp.take(patches, token_order, axis=0)
    local_rows = tokens.shape[0]
    mixed = jnp.dot(tokens, embed_weight, preferred_element_type=jnp.float32)
    inverse = lax.rsqrt(jnp.mean(mixed * mixed, axis=-1, keepdims=True) + 1e-06)
    normal = mixed * inverse
    hidden = (normal * norm_gain).astype(jnp.bfloat16)
    full_weight = lax.all_gather(qkv_weight, "seq", axis=0, tiled=True)
    local_width = full_weight.shape[2]
    head_local = local_width // HEAD_DIM
    flat_weight = full_weight.reshape(D, 3 * local_width)
    proj = jnp.dot(hidden, flat_weight, preferred_element_type=jnp.float32).astype(jnp.bfloat16)
    proj = proj.reshape(local_rows, 3, local_width)
    query = proj[:, 0]
    keys_all, values_all = (
        lax.all_gather(proj[:, 1], "seq", axis=0, tiled=True),
        lax.all_gather(proj[:, 2], "seq", axis=0, tiled=True),
    )
    cotan = grad_out[0]
    output_h, lse_h, delta_h, grad_q_h = lax.map(
        head_forward,
        (
            head_major(query, head_local),
            head_major(keys_all, head_local),
            head_major(values_all, head_local),
            head_major(cotan, head_local),
        ),
    )
    output = row_major(output_h)
    grad_q = row_major(grad_q_h)
    lse_all, delta_all = (
        lax.all_gather(jnp.transpose(lse_h), "seq", axis=0, tiled=True),
        lax.all_gather(jnp.transpose(delta_h), "seq", axis=0, tiled=True),
    )
    own_keys = head_major(proj[:, 1], head_local)
    own_values = head_major(proj[:, 2], head_local)
    query_piece = lax.all_gather(query, "seq", axis=0, tiled=True)
    cotan_piece = lax.all_gather(cotan, "seq", axis=0, tiled=True)
    lse_piece = jnp.transpose(lse_all)
    delta_piece = jnp.transpose(delta_all)
    key_add, value_add = lax.map(
        head_backward,
        (
            head_major(query_piece, head_local),
            head_major(cotan_piece, head_local),
            lse_piece,
            delta_piece,
            own_keys,
            own_values,
        ),
    )
    grad_k = row_major(key_add * HEAD_DIM ** (-0.5))
    grad_v = row_major(value_add)
    grads = (
        jnp.stack([grad_q, grad_k, grad_v], axis=1)
        .reshape(local_rows, 3 * local_width)
        .astype(jnp.bfloat16)
    )
    back_part = lax.dot_general(
        grads, flat_weight, (((1,), (1,)), ((), ())), preferred_element_type=jnp.float32
    )
    head_count_d = lax.axis_size("head")
    width_dev = D // head_count_d
    start_col = lax.axis_index("head") * width_dev
    normal_own = lax.dynamic_slice_in_dim(normal, start_col, width_dev, 1)
    gain_own = lax.dynamic_slice_in_dim(norm_gain, start_col, width_dev, 0)
    back_own = lax.psum_scatter(
        back_part.astype(jnp.bfloat16), "head", scatter_dimension=1, tiled=True
    ).astype(jnp.float32)
    scaled_own = back_own * gain_own
    inner_part = jnp.sum(scaled_own * normal_own, axis=-1, keepdims=True)
    inner = lax.psum(inner_part, "head") / D
    dmixed_own = inverse * (scaled_own - normal_own * inner)
    embed_part = jnp.dot(
        tokens.astype(jnp.float32).T,
        dmixed_own,
        preferred_element_type=jnp.float32,
        precision=lax.Precision.HIGHEST,
    )
    embed_grad = lax.psum(embed_part, ("grp", "seq"))
    attended = output.reshape(1, local_rows, local_width)
    return (attended, embed_grad)

def split2(value):
    high = value.astype(jnp.bfloat16)
    low = (value - high.astype(jnp.float32)).astype(jnp.bfloat16)
    return high, low


def mm(a, b, dims=((1,), (0,))):
    return lax.dot_general(a, b, (dims, ((), ())), preferred_element_type=jnp.float32)


NT = ((1,), (1,))
TN = ((0,), (0,))


def fused(
    groups, seq, feat_hbm, conv_hbm, bias_hbm, order_hbm, embed_hbm, gain_hbm, weight_hbm, cot_hbm,
    att_ref, grad_ref,
    feat_ref, conv_ref, bias_ref, order_ref, embed_ref, gain_ref, cot_ref,
    weight, mbuf, mrecv, cotpack, cots, orders, halo_own, halo_par, halo_in, lat_acc, patches, att, attin,
    hot_ref, gall, part, rrecv, quarter, gathered,
    in_sem, w_sem, m_send, m_recv, c_send, c_recv, o_send, o_recv, h_send, h_recv, l_send, l_recv,
    t_send, t_recv, g_send, g_recv, r_send, r_recv, f_send, f_recv, f_local,
):
    g, s, h = lax.axis_index("grp"), lax.axis_index("seq"), lax.axis_index("head")
    own_rows = cot_ref.shape[0]
    half_rows = own_rows // 2
    tokens_all = own_rows * seq
    depth = weight.shape[1]
    cols = weight.shape[2]
    patch = embed_ref.shape[0]
    half_patch = patch // 2
    width_model = embed_ref.shape[1]
    lat_ch = bias_ref.shape[1]
    pair = 2 * HEAD_DIM
    far = lambda off: lax.rem(s + off, seq)
    other = lambda off: lax.rem(g + off, groups)

    here_cols = pl.ds(pl.multiple_of(g * cols, 128), cols)
    w_copies = [
        pltpu.make_async_copy(weight_hbm.at[j, :, here_cols], weight.at[j], w_sem.at[j]) for j in range(3)
    ]
    in_copies = [
        pltpu.make_async_copy(src, dst, in_sem.at[i])
        for i, (src, dst) in enumerate(
            [
                (feat_hbm, feat_ref), (conv_hbm, conv_ref), (bias_hbm, bias_ref), (embed_hbm, embed_ref),
                (gain_hbm, gain_ref), (order_hbm, order_ref), (cot_hbm, cot_ref),
            ]
        )
    ]
    for c in in_copies + w_copies:
        c.start()
    barrier = pltpu.get_barrier_semaphore()
    everyone = [
        (dg, ds, dh) for ds in sorted(range(seq), key=lambda k: abs(k - seq // 2)) for dg in range(groups)
        for dh in range(2) if dg + ds + dh
    ]
    for dg, ds, dh in everyone:
        pl.semaphore_signal(
            barrier, inc=1, device_id=(other(dg), far(ds), lax.rem(h + dh, 2)), device_id_type=MESH
        )
    in_copies[0].wait()
    in_copies[1].wait()

    def remote(src, dst, send, recv, to):
        return pltpu.make_async_remote_copy(
            src_ref=src, dst_ref=dst, send_sem=send, recv_sem=recv, device_id=to, device_id_type=MESH
        )

    block = feat_ref.shape[0] // 4
    ri = lax.broadcasted_iota(jnp.int32, (4 * block, 4 * block), 0)
    ci = lax.broadcasted_iota(jnp.int32, (4 * block, 4 * block), 1)
    src_row = (ri // (2 * block)) * (2 * block) + 2 * lax.rem(ri, block) + lax.rem(ri // block, 2)
    sel = jnp.where(ci == src_row, 1.0, 0.0).astype(jnp.bfloat16)
    feat = mm(sel, feat_ref[...]).astype(jnp.bfloat16)
    jrow = lax.broadcasted_iota(jnp.int32, (block, 1), 0)

    def down(x):
        return jnp.where(jrow == 0, 0.0, pltpu.roll(x, 1, 0))

    def up(x):
        return jnp.where(jrow == block - 1, 0.0, pltpu.roll(x, block - 1, 0))

    z = {}
    for b in range(3):
        y = []
        for e in range(3):
            w_be = jnp.concatenate(
                [conv_ref[((a * 3 + b) * 3 + e) * lat_ch : ((a * 3 + b) * 3 + e + 1) * lat_ch, :] for a in range(3)],
                axis=0,
            )
            out = mm(feat, w_be, NT)
            y.append([[out[(2 * r + q) * block : (2 * r + q + 1) * block] for q in range(2)] for r in range(2)])
        for r in range(2):
            z[b, r, 0] = y[1][r][0] + y[2][r][1] + down(y[0][r][1])
            z[b, r, 1] = y[1][r][1] + y[0][r][0] + up(y[2][r][0])
    own = [z[1, 0, q] + z[2, 1, q] for q in range(2)] + [z[0, 0, q] + z[1, 1, q] for q in range(2)]
    edge = [jnp.where(h == 0, z[0, 1, q], z[2, 0, q]) for q in range(2)]
    par = [jnp.where(h == 0, edge[q], 0.0) for q in range(2)] + [jnp.where(h == 0, 0.0, edge[q]) for q in range(2)]
    for a in range(3):
        lanes = slice(a * lat_ch, (a + 1) * lat_ch)
        halo_own[a] = jnp.concatenate([x[:, lanes] for x in own], axis=1)
        halo_par[a] = jnp.concatenate([x[:, lanes] for x in par], axis=1)

    pl.semaphore_wait(barrier, 2 * groups * seq - 1)

    hops = [(0, 1, halo_par, 2), (1, 0, halo_own, 1), (1, 1, halo_par, 1), (2, 0, halo_own, 0), (2, 1, halo_par, 0)]

    def halo_copy(i):
        ds, dh, src, a = hops[i]
        return remote(
            src.at[a], halo_in.at[i], h_send.at[i], h_recv.at[i], (g, lax.rem(s + ds, seq), lax.rem(h + dh, 2))
        )

    halo_copy(0).start()
    for i in range(1, 5):
        pl.when(s + hops[i][0] < seq)(lambda i=i: halo_copy(i).start())

    for c in in_copies[2:]:
        c.wait()

    def order_copy(k):
        return remote(order_ref, orders.at[s], o_send.at[k - 1], o_recv.at[k - 1], (g, far(k), h))

    for k in range(1, seq):
        order_copy(k).start()
    orders[s] = order_ref[...]

    for i in range(groups * seq // 2):
        two = cot_ref[:, i * pair : (i + 1) * pair]
        for n in range(2):
            one = two[:, n * HEAD_DIM : (n + 1) * HEAD_DIM]
            cotpack[2 * i + n] = jnp.concatenate([one[:half_rows], one[half_rows:]], axis=1)
    mine = g * seq + s
    spots = [(dg, ds) for dg in range(groups) for ds in range(seq) if dg + ds]

    def cot_copy(k):
        dg, ds = spots[k]
        return remote(
            cotpack.at[other(dg) * seq + far(ds)], cots.at[mine], c_send.at[k], c_recv.at[k], (other(dg), far(ds), h)
        )

    for k in range(len(spots)):
        cot_copy(k).start()
    cots[mine] = cotpack[mine]

    own_cols = pl.ds(pl.multiple_of(s * depth, 128), depth)
    embed_own = embed_ref[:, own_cols].astype(jnp.float32)
    gain_own = gain_ref[:, own_cols]
    eg_high, eg_low = split2(embed_own * gain_own)
    eg = jnp.concatenate([eg_high, eg_low], axis=0)
    prods = []
    for j in range(3):
        w_copies[j].wait()
        prod = mm(eg, weight[j])
        prods.append(prod[:patch] + prod[patch:])
    for t in range(seq):
        q, k, v = (x[:, t * HEAD_DIM : (t + 1) * HEAD_DIM] for x in prods)
        mbuf[t, :patch] = jnp.concatenate([q, k], axis=1).astype(jnp.bfloat16)
        mbuf[t, patch:] = jnp.concatenate([v[:half_patch], v[half_patch:]], axis=1).astype(jnp.bfloat16)

    def m_copy(k):
        return remote(mbuf.at[far(k)], mrecv.at[k - 1], m_send.at[k - 1], m_recv.at[k - 1], (g, far(k), h))

    far_first = sorted(range(1, seq), key=lambda k: abs(k - seq // 2))
    for k in far_first[: seq // 2]:
        m_copy(k).start()

    halo_copy(0).wait_recv()
    lat_acc[...] = halo_own[2] + halo_in[0] + jnp.concatenate([bias_ref[...]] * 4, axis=1)
    for i in range(1, 5):

        def add(i=i):
            halo_copy(i).wait_recv()
            lat_acc[...] += halo_in[i]

        pl.when(s >= hops[i][0])(add)
    lat_at = (g * seq + s) * 2 + h
    patches[lat_at] = lat_acc[...].astype(jnp.bfloat16)

    def lat_copy(i):
        dg, ds, dh = everyone[i]
        return remote(
            patches.at[lat_at], patches.at[lat_at], l_send.at[i], l_recv.at[i],
            (other(dg), far(ds), lax.rem(h + dh, 2)),
        )

    for i in range(len(everyone)):
        lat_copy(i).start()
    for k in far_first[seq // 2 :]:
        m_copy(k).start()

    for k in range(1, seq):
        order_copy(k).wait_recv()
    row = jnp.concatenate([orders[t][:1] for t in range(seq)], axis=1).astype(jnp.float32)
    spread_order = jnp.transpose(jnp.broadcast_to(row, (128, tokens_all)))
    lane = lax.broadcasted_iota(jnp.int32, (tokens_all, 128), 1).astype(jnp.float32)
    for i in range(tokens_all // 128):
        hot_ref[:, i * 128 : (i + 1) * 128] = jnp.where(spread_order == lane + float(i * 128), 1.0, 0.0).astype(
            jnp.bfloat16
        )
    gram = mm(embed_ref[...], embed_ref[...], NT)
    gram_high, gram_rest = split2(gram)
    gram_mid, gram_low = split2(gram - gram_high.astype(jnp.float32))
    for k in range(len(spots)):
        cot_copy(k).wait_recv()

    for i in range(len(everyone)):
        lat_copy(i).wait_recv()
    tokens, inverse = [], []
    for c in range(groups):
        own_patches = patches[c * 2 * seq : (c + 1) * 2 * seq].reshape(tokens_all, patch)
        made = mm(hot_ref[...], own_patches)
        tok = made.astype(jnp.bfloat16)
        square = mm(tok, gram_high) + mm(tok, gram_mid) + mm(tok, gram_low)
        square = jnp.sum(square * made, axis=-1, keepdims=True)
        tokens.append(tok)
        inverse.append(lax.rsqrt(square / width_model + 1e-06))

    total = mbuf[s].astype(jnp.float32)
    for k in range(1, seq):
        m_copy(k).wait_recv()
        total = total + mrecv[k - 1].astype(jnp.float32)
    total = jnp.concatenate(
        [total[:patch], jnp.concatenate([total[patch:, :HEAD_DIM], total[patch:, HEAD_DIM:]], axis=0)], axis=1
    )
    m_high, m_low = split2(total)

    factor = HEAD_DIM ** (-0.5)
    made = jnp.zeros((patch, 4 * HEAD_DIM), jnp.float32)
    outs = []
    for c in range(groups):
        tok, inv = tokens[c], inverse[c]
        proj = (mm(tok, m_high) + mm(tok, m_low)) * inv
        low = proj.astype(jnp.bfloat16)
        lanes = lambda j: slice(j * HEAD_DIM, (j + 1) * HEAD_DIM)
        query, keys, values = low[:, lanes(0)], low[:, lanes(1)], low[:, lanes(2)]
        cotan = jnp.concatenate(
            [cots[c * seq + t][:, lanes(n)] for t in range(seq) for n in range(2)], axis=0
        )
        scores = mm(query, keys, NT) * factor
        top = jnp.max(scores, axis=-1, keepdims=True)
        expd = jnp.exp(scores - top)
        probs = expd * (1.0 / jnp.sum(expd, axis=-1, keepdims=True))
        probs_low = probs.astype(jnp.bfloat16)
        output = mm(probs_low, values).astype(jnp.bfloat16)
        delta = jnp.sum(cotan.astype(jnp.float32) * output.astype(jnp.float32), axis=-1, keepdims=True)
        dprob = mm(cotan, values, NT)
        dscore = (probs * (dprob - delta)).astype(jnp.bfloat16)
        outs.append(output)
        parts = [mm(dscore, keys) * factor, mm(dscore, query, TN) * factor, mm(probs_low, cotan, TN)]
        parts = [x.astype(jnp.bfloat16).astype(jnp.float32) for x in parts]
        inner = jnp.zeros((tokens_all, 1), jnp.float32)
        for j in range(3):
            inner = inner + jnp.sum(parts[j] * proj[:, lanes(j)], axis=-1, keepdims=True)
        rhs = [x * inv for x in parts] + [tok.astype(jnp.float32) * (inv * inv / width_model * inner)]
        rhs_high, rhs_low = split2(jnp.concatenate(rhs, axis=1))
        made = made + (mm(tok, rhs_high, TN) + mm(tok, rhs_low, TN))
    packed = [made[:, :pair]]
    for j in range(2, 4):
        piece = made[:, j * HEAD_DIM : (j + 1) * HEAD_DIM]
        packed.append(jnp.concatenate([piece[:half_patch], piece[half_patch:]], axis=1))
    gall[s] = jnp.concatenate(packed, axis=0).astype(jnp.bfloat16)

    beside = s + 1 - 2 * lax.rem(s, 2)
    hop = seq // 2

    def g_copy(k):
        if k < hop:
            source, to = s, far(2 * k)
        elif k == hop:
            source, to = s, beside
        else:
            source, to = far(seq - 2 * (k - hop)), beside
        return remote(gall.at[source], gall.at[source], g_send.at[k - 1], g_recv.at[k - 1], (g, to, h))

    for k in range(1, hop + 1):
        g_copy(k).start()

    for c in range(groups):
        for t in range(seq):
            one = outs[c][t * own_rows : (t + 1) * own_rows]
            att[c * seq + t] = jnp.concatenate([one[:half_rows], one[half_rows:]], axis=1)

    def att_copy(k):
        dg, ds = spots[k]
        return remote(
            att.at[other(dg) * seq + far(ds)], attin.at[mine], t_send.at[k], t_recv.at[k], (other(dg), far(ds), h)
        )

    attin[mine] = att[mine]

    for k in range(1, hop):
        g_copy(k).wait_recv()
        g_copy(hop + k).start()
    for k in range(len(spots)):
        att_copy(k).start()
    for k in range(hop, seq):
        g_copy(k).wait_recv()

    def spread(block, j):
        if j < 2:
            return block[:patch, j * HEAD_DIM : (j + 1) * HEAD_DIM]
        piece = block[patch + (j - 2) * half_patch : patch + (j - 1) * half_patch]
        return jnp.concatenate([piece[:, :HEAD_DIM], piece[:, HEAD_DIM:]], axis=0)

    back = jnp.zeros((patch, depth), jnp.float32)
    for j in range(3):
        all_heads = jnp.concatenate([spread(gall[t], j) for t in range(seq)], axis=1)
        back = back + mm(all_heads, weight[j], NT)
    outer = spread(gall[0], 3).astype(jnp.float32)
    for t in range(1, seq):
        outer = outer + spread(gall[t], 3).astype(jnp.float32)
    a_high, a_low = split2(outer)
    embed_low = embed_ref[:, own_cols]
    back = back * gain_own - (mm(a_high, embed_low) + mm(a_low, embed_low))
    rows = patch // (2 * groups)
    part[...] = back.reshape(2 * groups, rows, depth)
    rpeers = [(dg, dh) for dg in range(groups) for dh in range(2) if dg + dh]

    def r_copy(i):
        dg, dh = rpeers[i]
        og, oh = other(dg), lax.rem(h + dh, 2)
        return remote(part.at[og * 2 + oh], rrecv.at[i], r_send.at[i], r_recv.at[i], (og, s, oh))

    for i in range(len(rpeers)):
        r_copy(i).start()
    index = g * 2 + h
    done = part[index]
    for i in range(len(rpeers)):
        r_copy(i).wait_recv()
        done = done + rrecv[i]
    quarter[...] = done.astype(jnp.bfloat16)

    half = seq // 2
    owner = s // half
    slot = index * half + lax.rem(s, half)
    place = gathered.at[
        pl.ds(pl.multiple_of(index * rows, 16), rows), pl.ds(pl.multiple_of(lax.rem(s, half) * depth, 128), depth)
    ]

    def f_copy(k):
        dg, ds = k // seq, k % seq
        return remote(quarter, place, f_send.at[k], f_recv.at[slot], (other(dg), far(ds), owner))

    local = pltpu.make_async_copy(quarter, place, f_local)
    for k in sorted(range(1, groups * seq), key=lambda k: abs(k % seq - seq // 2)):
        f_copy(k).start()
    pl.when(owner != h)(lambda: f_copy(0).start())
    pl.when(owner == h)(lambda: local.start())

    def f_arrival(i):
        there = gathered.at[(i // half) * rows : (i // half + 1) * rows, (i % half) * depth : (i % half + 1) * depth]
        return remote(quarter, there, f_send.at[0], f_recv.at[i], (g, s, h))

    for k in range(len(spots)):
        att_copy(k).wait_recv()
    for i in range(groups * seq // 2):
        both = [attin[2 * i], attin[2 * i + 1]]
        for n in range(2):
            att_ref[n * half_rows : (n + 1) * half_rows, i * pair : (i + 1) * pair] = jnp.concatenate(
                [x[:, n * HEAD_DIM : (n + 1) * HEAD_DIM] for x in both], axis=1
            )
    for k in range(1, seq):
        order_copy(k).wait_send()
        m_copy(k).wait_send()
        g_copy(k).wait_send()
    for k in range(len(spots)):
        cot_copy(k).wait_send()
        att_copy(k).wait_send()
    halo_copy(0).wait_send()
    for i in range(1, 5):
        pl.when(s + hops[i][0] < seq)(lambda i=i: halo_copy(i).wait_send())
    for i in range(len(everyone)):
        lat_copy(i).wait_send()
    for i in range(len(rpeers)):
        r_copy(i).wait_send()
    for k in range(1, groups * seq):
        f_copy(k).wait_send()
    pl.when(owner != h)(lambda: f_copy(0).wait_send())
    pl.when(owner == h)(lambda: local.wait())
    for i in range(2 * groups * half):
        pl.when(jnp.logical_or(owner != h, slot != i))(lambda i=i: f_arrival(i).wait_recv())
    grad_ref[...] = gathered[...].astype(jnp.float32)


def fast_device(groups, seq, *operands):
    features, conv_weight, conv_bias, token_order, embed_weight, norm_gain, qkv_weight, grad_out = operands
    channels, lat_ch = conv_weight.shape[-2:]
    depth, _, width = qkv_weight.shape
    patch, model = embed_weight.shape
    own_rows = token_order.shape[0]
    cols = width // groups
    block = features.shape[2] * features.shape[3] // 4
    tokens_all = own_rows * seq
    pair = 2 * HEAD_DIM
    f32, b16 = jnp.float32, jnp.bfloat16
    vmem = pl.BlockSpec(memory_space=pltpu.VMEM)
    dma = pltpu.SemaphoreType.DMA
    rows = patch // (2 * groups)
    spots, everyone = groups * seq, 2 * groups * seq
    pairs = (
        [7, 3] + [seq - 1] * 2 + [spots - 1] * 2 + [seq - 1] * 2 + [5] * 2 + [everyone - 1] * 2 + [spots - 1] * 2
        + [seq - 1] * 2 + [2 * groups - 1] * 2 + [spots] * 2
    )
    attended, embed_grad = pl.pallas_call(
        functools.partial(fused, groups, seq),
        out_shape=(
            jax.ShapeDtypeStruct((own_rows, width), b16),
            jax.ShapeDtypeStruct((patch, model // 2), f32),
        ),
        in_specs=[pl.BlockSpec(memory_space=pltpu.HBM)] * 8,
        out_specs=(vmem, vmem),
        scratch_shapes=[
            pltpu.VMEM((4 * block, channels), b16),
            pltpu.VMEM((27 * lat_ch, channels), b16),
            pltpu.VMEM((1, lat_ch), f32),
            pltpu.VMEM((1, own_rows), jnp.int32),
            pltpu.VMEM((patch, model), b16),
            pltpu.VMEM((1, model), f32),
            pltpu.VMEM((own_rows, width), b16),
            pltpu.VMEM((3, depth, cols), b16),
            pltpu.VMEM((seq, 3 * patch // 2, pair), b16),
            pltpu.VMEM((seq - 1, 3 * patch // 2, pair), b16),
            pltpu.VMEM((spots, own_rows // 2, pair), b16),
            pltpu.VMEM((spots, own_rows // 2, pair), b16),
            pltpu.VMEM((seq, 1, own_rows), jnp.int32),
            pltpu.VMEM((3, block, patch), f32),
            pltpu.VMEM((3, block, patch), f32),
            pltpu.VMEM((5, block, patch), f32),
            pltpu.VMEM((block, patch), f32),
            pltpu.VMEM((everyone, block, patch), b16),
            pltpu.VMEM((spots, own_rows // 2, pair), b16),
            pltpu.VMEM((spots, own_rows // 2, pair), b16),
            pltpu.VMEM((tokens_all, tokens_all), b16),
            pltpu.VMEM((seq, 2 * patch, pair), b16),
            pltpu.VMEM((2 * groups, rows, depth), f32),
            pltpu.VMEM((2 * groups - 1, rows, depth), f32),
            pltpu.VMEM((rows, depth), b16),
            pltpu.VMEM((patch, model // 2), b16),
        ]
        + [dma((n,)) for n in pairs]
        + [dma],
        compiler_params=pltpu.CompilerParams(collective_id=0, has_side_effects=True),
    )(
        features.reshape(4 * block, channels),
        jnp.transpose(conv_weight, (0, 1, 2, 4, 3)).reshape(-1, channels),
        conv_bias.reshape(1, lat_ch),
        token_order.reshape(1, own_rows),
        embed_weight,
        norm_gain.reshape(1, model),
        jnp.transpose(qkv_weight, (1, 0, 2)),
        grad_out[0],
    )
    return attended[None], embed_grad


def fits(mesh, features, conv_weight, embed_weight, qkv_weight, token_order):
    groups, seq, heads = (mesh.shape[axis] for axis in ("grp", "seq", "head"))
    clips, frames, rows, columns, _ = features.shape
    width = qkv_weight.shape[2] // heads
    depth = qkv_weight.shape[0] // seq
    patch = embed_weight.shape[0]
    return (
        heads == 2
        and clips == groups
        and frames == seq
        and seq % 2 == 0
        and rows == 2 * heads
        and columns % 32 == 0
        and width == groups * seq * HEAD_DIM
        and (seq * HEAD_DIM) % 128 == 0
        and depth % 128 == 0
        and patch == 4 * conv_weight.shape[-1]
        and patch == HEAD_DIM
        and patch % (16 * groups) == 0
        and token_order.shape[0] == seq * columns
        and token_order.shape[0] % (32 * seq) == 0
        and token_order.shape[0] % 128 == 0
    )


def solution(mesh):
    placed = (
        P("grp", "seq", "head", None, None),
        P(),
        P(),
        P("seq"),
        P(),
        P(),
        P("seq", None, "head"),
        P("grp", "seq", "head"),
    )

    def run(features, conv_weight, conv_bias, token_order, embed_weight, norm_gain, qkv_weight, grad_out):
        body = per_device
        if fits(mesh, features, conv_weight, embed_weight, qkv_weight, token_order):
            body = functools.partial(fast_device, mesh.shape["grp"], mesh.shape["seq"])
        return jax.shard_map(
            body,
            mesh=mesh,
            in_specs=placed,
            out_specs=(P("grp", "seq", "head"), P(None, "head")),
            check_vma=False,
        )(features, conv_weight, conv_bias, token_order, embed_weight, norm_gain, qkv_weight, grad_out)

    return run
```

```python
import functools

import jax
import jax.numpy as jnp
from jax import lax
from jax.experimental import pallas as pl
from jax.experimental.pallas import tpu as pltpu
from jax.sharding import PartitionSpec as P

D = 3072
HEAD_DIM = 64
MESH = pl.DeviceIdType.MESH


def shifted(value, axis, steps):
    count = lax.axis_size(axis)
    leading, last = (max(0, -steps), min(count, count - steps))
    return lax.ppermute(value, axis, [(source, source + steps) for source in range(leading, last)])


def extended(block, sides, width):
    for axis, dim in sides:
        count = lax.axis_size(axis)
        forward = [(i, i + 1) for i in range(count - 1)]
        backward = [(target, source) for source, target in forward]
        low = lax.ppermute(
            lax.slice_in_dim(block, block.shape[dim] - width, None, axis=dim), axis, forward
        )
        high = lax.ppermute(lax.slice_in_dim(block, 0, width, axis=dim), axis, backward)
        block = jnp.concatenate([low, block, high], axis=dim)
    return block


def patchify(latent):
    frames, rows, columns, channels = latent.shape
    blocks = latent.reshape(frames, rows // 2, 2, columns // 2, 2, channels)
    blocks = jnp.transpose(blocks, (0, 1, 3, 2, 4, 5))
    return blocks.reshape(frames * (rows // 2) * (columns // 2), 4 * channels)


def encode_tile(tile, conv_weight, conv_bias):
    frames, rows, columns, channels = tile.shape
    hops = (frames + 1) // frames
    earlier = []
    for hop in range(hops, 0, -1):
        earlier.append(shifted(tile, "seq", hop))
    stacked = jnp.concatenate(earlier + [tile], axis=0)
    padded = extended(stacked, (("head", 1),), 1)
    padded = jnp.pad(padded, ((0, 0), (0, 0), (1, 1), (0, 0)))
    total = jnp.zeros((frames * rows * columns, conv_weight.shape[-1]), jnp.float32) + conv_bias
    for a in range(3):
        for b in range(3):
            for e in range(3):
                piece = padded[a : a + frames, b : b + rows, e : e + columns].reshape(-1, channels)
                total = total + jnp.dot(
                    piece, conv_weight[a, b, e], preferred_element_type=jnp.float32
                )
    return total.astype(jnp.bfloat16).reshape(frames, rows, columns, conv_weight.shape[-1])


def head_major(matrix, head_local):
    count = matrix.shape[0]
    return jnp.transpose(matrix.reshape(count, head_local, HEAD_DIM), (1, 0, 2))


def row_major(stacked):
    heads_here, count, size = stacked.shape
    return jnp.transpose(stacked, (1, 0, 2)).reshape(count, heads_here * size)


def head_forward(operands):
    query, keys, values, cotan = operands
    factor = HEAD_DIM ** (-0.5)
    scores = jnp.dot(query, keys.T, preferred_element_type=jnp.float32) * factor
    top = jnp.max(scores, axis=-1, keepdims=True)
    lse = top + jnp.log(jnp.sum(jnp.exp(scores - top), axis=-1, keepdims=True))
    probs = jnp.exp(scores - lse)
    probs_low = probs.astype(jnp.bfloat16)
    output = jnp.dot(probs_low, values, preferred_element_type=jnp.float32).astype(jnp.bfloat16)
    delta = jnp.sum(cotan.astype(jnp.float32) * output.astype(jnp.float32), axis=-1, keepdims=True)
    dprob = jnp.dot(cotan, values.T, preferred_element_type=jnp.float32)
    dscore = (probs * (dprob - delta)).astype(jnp.bfloat16)
    grad_q = jnp.dot(dscore, keys, preferred_element_type=jnp.float32) * factor
    return (output, lse[:, 0], delta[:, 0], grad_q)


def head_backward(operands):
    query, cotan, lse_piece, delta_piece, own_keys, own_values = operands
    factor = HEAD_DIM ** (-0.5)
    scores = jnp.dot(query, own_keys.T, preferred_element_type=jnp.float32) * factor
    probs = jnp.exp(scores - lse_piece[:, None])
    value_add = jnp.dot(probs.astype(jnp.bfloat16).T, cotan, preferred_element_type=jnp.float32)
    dprob = jnp.dot(cotan, own_values.T, preferred_element_type=jnp.float32)
    dscore = (probs * (dprob - delta_piece[:, None])).astype(jnp.bfloat16)
    key_add = jnp.dot(dscore.T, query, preferred_element_type=jnp.float32)
    return (key_add, value_add)


def per_device(
    features, conv_weight, conv_bias, token_order, embed_weight, norm_gain, qkv_weight, grad_out
):
    tile = encode_tile(features[0], conv_weight, conv_bias)
    all_rows = lax.all_gather(tile, "head", axis=1, tiled=True)
    whole = lax.all_gather(all_rows, "seq", axis=0, tiled=True)
    patches = patchify(whole)
    tokens = jnp.take(patches, token_order, axis=0)
    local_rows = tokens.shape[0]
    mixed = jnp.dot(tokens, embed_weight, preferred_element_type=jnp.float32)
    inverse = lax.rsqrt(jnp.mean(mixed * mixed, axis=-1, keepdims=True) + 1e-06)
    normal = mixed * inverse
    hidden = (normal * norm_gain).astype(jnp.bfloat16)
    full_weight = lax.all_gather(qkv_weight, "seq", axis=0, tiled=True)
    local_width = full_weight.shape[2]
    head_local = local_width // HEAD_DIM
    flat_weight = full_weight.reshape(D, 3 * local_width)
    proj = jnp.dot(hidden, flat_weight, preferred_element_type=jnp.float32).astype(jnp.bfloat16)
    proj = proj.reshape(local_rows, 3, local_width)
    query = proj[:, 0]
    keys_all, values_all = (
        lax.all_gather(proj[:, 1], "seq", axis=0, tiled=True),
        lax.all_gather(proj[:, 2], "seq", axis=0, tiled=True),
    )
    cotan = grad_out[0]
    output_h, lse_h, delta_h, grad_q_h = lax.map(
        head_forward,
        (
            head_major(query, head_local),
            head_major(keys_all, head_local),
            head_major(values_all, head_local),
            head_major(cotan, head_local),
        ),
    )
    output = row_major(output_h)
    grad_q = row_major(grad_q_h)
    lse_all, delta_all = (
        lax.all_gather(jnp.transpose(lse_h), "seq", axis=0, tiled=True),
        lax.all_gather(jnp.transpose(delta_h), "seq", axis=0, tiled=True),
    )
    own_keys = head_major(proj[:, 1], head_local)
    own_values = head_major(proj[:, 2], head_local)
    query_piece = lax.all_gather(query, "seq", axis=0, tiled=True)
    cotan_piece = lax.all_gather(cotan, "seq", axis=0, tiled=True)
    lse_piece = jnp.transpose(lse_all)
    delta_piece = jnp.transpose(delta_all)
    key_add, value_add = lax.map(
        head_backward,
        (
            head_major(query_piece, head_local),
            head_major(cotan_piece, head_local),
            lse_piece,
            delta_piece,
            own_keys,
            own_values,
        ),
    )
    grad_k = row_major(key_add * HEAD_DIM ** (-0.5))
    grad_v = row_major(value_add)
    grads = (
        jnp.stack([grad_q, grad_k, grad_v], axis=1)
        .reshape(local_rows, 3 * local_width)
        .astype(jnp.bfloat16)
    )
    back_part = lax.dot_general(
        grads, flat_weight, (((1,), (1,)), ((), ())), preferred_element_type=jnp.float32
    )
    head_count_d = lax.axis_size("head")
    width_dev = D // head_count_d
    start_col = lax.axis_index("head") * width_dev
    normal_own = lax.dynamic_slice_in_dim(normal, start_col, width_dev, 1)
    gain_own = lax.dynamic_slice_in_dim(norm_gain, start_col, width_dev, 0)
    back_own = lax.psum_scatter(
        back_part.astype(jnp.bfloat16), "head", scatter_dimension=1, tiled=True
    ).astype(jnp.float32)
    scaled_own = back_own * gain_own
    inner_part = jnp.sum(scaled_own * normal_own, axis=-1, keepdims=True)
    inner = lax.psum(inner_part, "head") / D
    dmixed_own = inverse * (scaled_own - normal_own * inner)
    embed_part = jnp.dot(
        tokens.astype(jnp.float32).T,
        dmixed_own,
        preferred_element_type=jnp.float32,
        precision=lax.Precision.HIGHEST,
    )
    embed_grad = lax.psum(embed_part, ("grp", "seq"))
    attended = output.reshape(1, local_rows, local_width)
    return (attended, embed_grad)

def split2(value):
    high = value.astype(jnp.bfloat16)
    low = (value - high.astype(jnp.float32)).astype(jnp.bfloat16)
    return high, low


def mm(a, b, dims=((1,), (0,))):
    return lax.dot_general(a, b, (dims, ((), ())), preferred_element_type=jnp.float32)


NT = ((1,), (1,))
TN = ((0,), (0,))


def fused(
    groups, seq, feat_hbm, conv_hbm, bias_hbm, order_hbm, embed_hbm, gain_hbm, weight_hbm, cot_hbm,
    att_ref, grad_ref,
    feat_ref, conv_ref, bias_ref, order_ref, embed_ref, gain_ref, cot_ref,
    weight, mbuf, mrecv, cotpack, cots, orders, halo_own, halo_par, halo_in, lat_acc, patches, att, attin,
    hot_ref, gall, part, rrecv, quarter, gathered,
    in_sem, w_sem, m_send, m_recv, c_send, c_recv, o_send, o_recv, h_send, h_recv, l_send, l_recv,
    t_send, t_recv, g_send, g_recv, r_send, r_recv, f_send, f_recv, f_local,
):
    g, s, h = lax.axis_index("grp"), lax.axis_index("seq"), lax.axis_index("head")
    own_rows = cot_ref.shape[0]
    half_rows = own_rows // 2
    tokens_all = own_rows * seq
    depth = weight.shape[1]
    cols = weight.shape[2]
    patch = embed_ref.shape[0]
    half_patch = patch // 2
    width_model = embed_ref.shape[1]
    lat_ch = bias_ref.shape[1]
    pair = 2 * HEAD_DIM
    far = lambda off: lax.rem(s + off, seq)
    other = lambda off: lax.rem(g + off, groups)

    here_cols = pl.ds(pl.multiple_of(g * cols, 128), cols)
    w_copies = [
        pltpu.make_async_copy(weight_hbm.at[j, :, here_cols], weight.at[j], w_sem.at[j]) for j in range(3)
    ]
    in_copies = [
        pltpu.make_async_copy(src, dst, in_sem.at[i])
        for i, (src, dst) in enumerate(
            [
                (feat_hbm, feat_ref), (conv_hbm, conv_ref), (bias_hbm, bias_ref), (embed_hbm, embed_ref),
                (gain_hbm, gain_ref), (order_hbm, order_ref), (cot_hbm, cot_ref),
            ]
        )
    ]
    for c in in_copies + w_copies:
        c.start()
    barrier = pltpu.get_barrier_semaphore()
    everyone = [
        (dg, ds, dh) for ds in sorted(range(seq), key=lambda k: abs(k - seq // 2)) for dg in range(groups)
        for dh in range(2) if dg + ds + dh
    ]
    for dg, ds, dh in everyone:
        pl.semaphore_signal(
            barrier, inc=1, device_id=(other(dg), far(ds), lax.rem(h + dh, 2)), device_id_type=MESH
        )
    in_copies[0].wait()
    in_copies[1].wait()

    def remote(src, dst, send, recv, to):
        return pltpu.make_async_remote_copy(
            src_ref=src, dst_ref=dst, send_sem=send, recv_sem=recv, device_id=to, device_id_type=MESH
        )

    block = feat_ref.shape[0] // 4
    ri = lax.broadcasted_iota(jnp.int32, (4 * block, 4 * block), 0)
    ci = lax.broadcasted_iota(jnp.int32, (4 * block, 4 * block), 1)
    src_row = (ri // (2 * block)) * (2 * block) + 2 * lax.rem(ri, block) + lax.rem(ri // block, 2)
    sel = jnp.where(ci == src_row, 1.0, 0.0).astype(jnp.bfloat16)
    feat = mm(sel, feat_ref[...]).astype(jnp.bfloat16)
    jrow = lax.broadcasted_iota(jnp.int32, (block, 1), 0)

    def down(x):
        return jnp.where(jrow == 0, 0.0, pltpu.roll(x, 1, 0))

    def up(x):
        return jnp.where(jrow == block - 1, 0.0, pltpu.roll(x, block - 1, 0))

    z = {}
    for b in range(3):
        y = []
        for e in range(3):
            w_be = jnp.concatenate(
                [conv_ref[((a * 3 + b) * 3 + e) * lat_ch : ((a * 3 + b) * 3 + e + 1) * lat_ch, :] for a in range(3)],
                axis=0,
            )
            out = mm(feat, w_be, NT)
            y.append([[out[(2 * r + q) * block : (2 * r + q + 1) * block] for q in range(2)] for r in range(2)])
        for r in range(2):
            z[b, r, 0] = y[1][r][0] + y[2][r][1] + down(y[0][r][1])
            z[b, r, 1] = y[1][r][1] + y[0][r][0] + up(y[2][r][0])
    own = [z[1, 0, q] + z[2, 1, q] for q in range(2)] + [z[0, 0, q] + z[1, 1, q] for q in range(2)]
    edge = [jnp.where(h == 0, z[0, 1, q], z[2, 0, q]) for q in range(2)]
    par = [jnp.where(h == 0, edge[q], 0.0) for q in range(2)] + [jnp.where(h == 0, 0.0, edge[q]) for q in range(2)]
    for a in range(3):
        lanes = slice(a * lat_ch, (a + 1) * lat_ch)
        halo_own[a] = jnp.concatenate([x[:, lanes] for x in own], axis=1)
        halo_par[a] = jnp.concatenate([x[:, lanes] for x in par], axis=1)

    pl.semaphore_wait(barrier, 2 * groups * seq - 1)

    hops = [(0, 1, halo_par, 2), (1, 0, halo_own, 1), (1, 1, halo_par, 1), (2, 0, halo_own, 0), (2, 1, halo_par, 0)]

    def halo_copy(i):
        ds, dh, src, a = hops[i]
        return remote(
            src.at[a], halo_in.at[i], h_send.at[i], h_recv.at[i], (g, lax.rem(s + ds, seq), lax.rem(h + dh, 2))
        )

    halo_copy(0).start()
    for i in range(1, 5):
        pl.when(s + hops[i][0] < seq)(lambda i=i: halo_copy(i).start())

    for c in in_copies[2:]:
        c.wait()

    def order_copy(k):
        return remote(order_ref, orders.at[s], o_send.at[k - 1], o_recv.at[k - 1], (g, far(k), h))

    for k in range(1, seq):
        order_copy(k).start()
    orders[s] = order_ref[...]

    for i in range(groups * seq // 2):
        two = cot_ref[:, i * pair : (i + 1) * pair]
        for n in range(2):
            one = two[:, n * HEAD_DIM : (n + 1) * HEAD_DIM]
            cotpack[2 * i + n] = jnp.concatenate([one[:half_rows], one[half_rows:]], axis=1)
    mine = g * seq + s
    spots = [(dg, ds) for dg in range(groups) for ds in range(seq) if dg + ds]

    def cot_copy(k):
        dg, ds = spots[k]
        return remote(
            cotpack.at[other(dg) * seq + far(ds)], cots.at[mine], c_send.at[k], c_recv.at[k], (other(dg), far(ds), h)
        )

    for k in range(len(spots)):
        cot_copy(k).start()
    cots[mine] = cotpack[mine]

    own_cols = pl.ds(pl.multiple_of(s * depth, 128), depth)
    embed_own = embed_ref[:, own_cols].astype(jnp.float32)
    gain_own = gain_ref[:, own_cols]
    eg_high, eg_low = split2(embed_own * gain_own)
    eg = jnp.concatenate([eg_high, eg_low], axis=0)
    prods = []
    for j in range(3):
        w_copies[j].wait()
        prod = mm(eg, weight[j])
        prods.append(prod[:patch] + prod[patch:])
    for t in range(seq):
        q, k, v = (x[:, t * HEAD_DIM : (t + 1) * HEAD_DIM] for x in prods)
        mbuf[t, :patch] = jnp.concatenate([q, k], axis=1).astype(jnp.bfloat16)
        mbuf[t, patch:] = jnp.concatenate([v[:half_patch], v[half_patch:]], axis=1).astype(jnp.bfloat16)

    def m_copy(k):
        return remote(mbuf.at[far(k)], mrecv.at[k - 1], m_send.at[k - 1], m_recv.at[k - 1], (g, far(k), h))

    far_first = sorted(range(1, seq), key=lambda k: abs(k - seq // 2))
    for k in far_first[: seq // 2]:
        m_copy(k).start()

    halo_copy(0).wait_recv()
    lat_acc[...] = halo_own[2] + halo_in[0] + jnp.concatenate([bias_ref[...]] * 4, axis=1)
    for i in range(1, 5):

        def add(i=i):
            halo_copy(i).wait_recv()
            lat_acc[...] += halo_in[i]

        pl.when(s >= hops[i][0])(add)
    lat_at = (g * seq + s) * 2 + h
    patches[lat_at] = lat_acc[...].astype(jnp.bfloat16)

    def lat_copy(i):
        dg, ds, dh = everyone[i]
        return remote(
            patches.at[lat_at], patches.at[lat_at], l_send.at[i], l_recv.at[i],
            (other(dg), far(ds), lax.rem(h + dh, 2)),
        )

    for i in range(len(everyone)):
        lat_copy(i).start()
    for k in far_first[seq // 2 :]:
        m_copy(k).start()

    for k in range(1, seq):
        order_copy(k).wait_recv()
    row = jnp.concatenate([orders[t][:1] for t in range(seq)], axis=1).astype(jnp.float32)
    spread_order = jnp.transpose(jnp.broadcast_to(row, (128, tokens_all)))
    lane = lax.broadcasted_iota(jnp.int32, (tokens_all, 128), 1).astype(jnp.float32)
    for i in range(tokens_all // 128):
        hot_ref[:, i * 128 : (i + 1) * 128] = jnp.where(spread_order == lane + float(i * 128), 1.0, 0.0).astype(
            jnp.bfloat16
        )
    gram = mm(embed_ref[...], embed_ref[...], NT)
    gram_high, gram_rest = split2(gram)
    gram_mid, gram_low = split2(gram - gram_high.astype(jnp.float32))
    for k in range(len(spots)):
        cot_copy(k).wait_recv()

    for i in range(len(everyone)):
        lat_copy(i).wait_recv()
    tokens, inverse = [], []
    for c in range(groups):
        own_patches = patches[c * 2 * seq : (c + 1) * 2 * seq].reshape(tokens_all, patch)
        made = mm(hot_ref[...], own_patches)
        tok = made.astype(jnp.bfloat16)
        square = mm(tok, gram_high) + mm(tok, gram_mid) + mm(tok, gram_low)
        square = jnp.sum(square * made, axis=-1, keepdims=True)
        tokens.append(tok)
        inverse.append(lax.rsqrt(square / width_model + 1e-06))

    total = mbuf[s].astype(jnp.float32)
    for k in range(1, seq):
        m_copy(k).wait_recv()
        total = total + mrecv[k - 1].astype(jnp.float32)
    total = jnp.concatenate(
        [total[:patch], jnp.concatenate([total[patch:, :HEAD_DIM], total[patch:, HEAD_DIM:]], axis=0)], axis=1
    )
    m_high, m_low = split2(total)

    factor = HEAD_DIM ** (-0.5)
    made = jnp.zeros((patch, 4 * HEAD_DIM), jnp.float32)
    outs = []
    for c in range(groups):
        tok, inv = tokens[c], inverse[c]
        proj = (mm(tok, m_high) + mm(tok, m_low)) * inv
        low = proj.astype(jnp.bfloat16)
        lanes = lambda j: slice(j * HEAD_DIM, (j + 1) * HEAD_DIM)
        query, keys, values = low[:, lanes(0)], low[:, lanes(1)], low[:, lanes(2)]
        cotan = jnp.concatenate(
            [cots[c * seq + t][:, lanes(n)] for t in range(seq) for n in range(2)], axis=0
        )
        scores = mm(query, keys, NT) * factor
        top = jnp.max(scores, axis=-1, keepdims=True)
        expd = jnp.exp(scores - top)
        probs = expd * (1.0 / jnp.sum(expd, axis=-1, keepdims=True))
        probs_low = probs.astype(jnp.bfloat16)
        output = mm(probs_low, values).astype(jnp.bfloat16)
        delta = jnp.sum(cotan.astype(jnp.float32) * output.astype(jnp.float32), axis=-1, keepdims=True)
        dprob = mm(cotan, values, NT)
        dscore = (probs * (dprob - delta)).astype(jnp.bfloat16)
        outs.append(output)
        parts = [mm(dscore, keys) * factor, mm(dscore, query, TN) * factor, mm(probs_low, cotan, TN)]
        parts = [x.astype(jnp.bfloat16).astype(jnp.float32) for x in parts]
        inner = jnp.zeros((tokens_all, 1), jnp.float32)
        for j in range(3):
            inner = inner + jnp.sum(parts[j] * proj[:, lanes(j)], axis=-1, keepdims=True)
        rhs = [x * inv for x in parts] + [tok.astype(jnp.float32) * (inv * inv / width_model * inner)]
        rhs_high, rhs_low = split2(jnp.concatenate(rhs, axis=1))
        made = made + (mm(tok, rhs_high, TN) + mm(tok, rhs_low, TN))
    packed = [made[:, :pair]]
    for j in range(2, 4):
        piece = made[:, j * HEAD_DIM : (j + 1) * HEAD_DIM]
        packed.append(jnp.concatenate([piece[:half_patch], piece[half_patch:]], axis=1))
    gall[s] = jnp.concatenate(packed, axis=0).astype(jnp.bfloat16)

    beside = s + 1 - 2 * lax.rem(s, 2)
    hop = seq // 2

    def g_copy(k):
        if k < hop:
            source, to = s, far(2 * k)
        elif k == hop:
            source, to = s, beside
        else:
            source, to = far(seq - 2 * (k - hop)), beside
        return remote(gall.at[source], gall.at[source], g_send.at[k - 1], g_recv.at[k - 1], (g, to, h))

    for k in range(1, hop + 1):
        g_copy(k).start()

    for c in range(groups):
        for t in range(seq):
            one = outs[c][t * own_rows : (t + 1) * own_rows]
            att[c * seq + t] = jnp.concatenate([one[:half_rows], one[half_rows:]], axis=1)

    def att_copy(k):
        dg, ds = spots[k]
        return remote(
            att.at[other(dg) * seq + far(ds)], attin.at[mine], t_send.at[k], t_recv.at[k], (other(dg), far(ds), h)
        )

    attin[mine] = att[mine]

    for k in range(1, hop):
        g_copy(k).wait_recv()
        g_copy(hop + k).start()
    for k in range(len(spots)):
        att_copy(k).start()
    for k in range(hop, seq):
        g_copy(k).wait_recv()

    def spread(block, j):
        if j < 2:
            return block[:patch, j * HEAD_DIM : (j + 1) * HEAD_DIM]
        piece = block[patch + (j - 2) * half_patch : patch + (j - 1) * half_patch]
        return jnp.concatenate([piece[:, :HEAD_DIM], piece[:, HEAD_DIM:]], axis=0)

    back = jnp.zeros((patch, depth), jnp.float32)
    for j in range(3):
        all_heads = jnp.concatenate([spread(gall[t], j) for t in range(seq)], axis=1)
        back = back + mm(all_heads, weight[j], NT)
    outer = spread(gall[0], 3).astype(jnp.float32)
    for t in range(1, seq):
        outer = outer + spread(gall[t], 3).astype(jnp.float32)
    a_high, a_low = split2(outer)
    embed_low = embed_ref[:, own_cols]
    back = back * gain_own - (mm(a_high, embed_low) + mm(a_low, embed_low))
    rows = patch // (2 * groups)
    part[...] = back.reshape(2 * groups, rows, depth)
    rpeers = [(dg, dh) for dg in range(groups) for dh in range(2) if dg + dh]

    def r_copy(i):
        dg, dh = rpeers[i]
        og, oh = other(dg), lax.rem(h + dh, 2)
        return remote(part.at[og * 2 + oh], rrecv.at[i], r_send.at[i], r_recv.at[i], (og, s, oh))

    for i in range(len(rpeers)):
        r_copy(i).start()
    index = g * 2 + h
    done = part[index]
    for i in range(len(rpeers)):
        r_copy(i).wait_recv()
        done = done + rrecv[i]
    quarter[...] = done.astype(jnp.bfloat16)

    half = seq // 2
    owner = s // half
    slot = index * half + lax.rem(s, half)
    place = gathered.at[
        pl.ds(pl.multiple_of(index * rows, 16), rows), pl.ds(pl.multiple_of(lax.rem(s, half) * depth, 128), depth)
    ]

    def f_copy(k):
        dg, ds = k // seq, k % seq
        return remote(quarter, place, f_send.at[k], f_recv.at[slot], (other(dg), far(ds), owner))

    local = pltpu.make_async_copy(quarter, place, f_local)
    for k in sorted(range(1, groups * seq), key=lambda k: abs(k % seq - seq // 2)):
        f_copy(k).start()
    pl.when(owner != h)(lambda: f_copy(0).start())
    pl.when(owner == h)(lambda: local.start())

    def f_arrival(i):
        there = gathered.at[(i // half) * rows : (i // half + 1) * rows, (i % half) * depth : (i % half + 1) * depth]
        return remote(quarter, there, f_send.at[0], f_recv.at[i], (g, s, h))

    for k in range(len(spots)):
        att_copy(k).wait_recv()
    for i in range(groups * seq // 2):
        both = [attin[2 * i], attin[2 * i + 1]]
        for n in range(2):
            att_ref[n * half_rows : (n + 1) * half_rows, i * pair : (i + 1) * pair] = jnp.concatenate(
                [x[:, n * HEAD_DIM : (n + 1) * HEAD_DIM] for x in both], axis=1
            )
    for k in range(1, seq):
        order_copy(k).wait_send()
        m_copy(k).wait_send()
        g_copy(k).wait_send()
    for k in range(len(spots)):
        cot_copy(k).wait_send()
        att_copy(k).wait_send()
    halo_copy(0).wait_send()
    for i in range(1, 5):
        pl.when(s + hops[i][0] < seq)(lambda i=i: halo_copy(i).wait_send())
    for i in range(len(everyone)):
        lat_copy(i).wait_send()
    for i in range(len(rpeers)):
        r_copy(i).wait_send()
    for k in range(1, groups * seq):
        f_copy(k).wait_send()
    pl.when(owner != h)(lambda: f_copy(0).wait_send())
    pl.when(owner == h)(lambda: local.wait())
    for i in range(2 * groups * half):
        pl.when(jnp.logical_or(owner != h, slot != i))(lambda i=i: f_arrival(i).wait_recv())
    grad_ref[...] = gathered[...]


def finish(att_in, grad_in, att_out, grad_out):
    att_out[...] = att_in[...]
    grad_out[...] = grad_in[...].astype(jnp.float32)


def fast_device(groups, seq, *operands):
    features, conv_weight, conv_bias, token_order, embed_weight, norm_gain, qkv_weight, grad_out = operands
    channels, lat_ch = conv_weight.shape[-2:]
    depth, _, width = qkv_weight.shape
    patch, model = embed_weight.shape
    own_rows = token_order.shape[0]
    cols = width // groups
    block = features.shape[2] * features.shape[3] // 4
    tokens_all = own_rows * seq
    pair = 2 * HEAD_DIM
    f32, b16 = jnp.float32, jnp.bfloat16
    vmem = pl.BlockSpec(memory_space=pltpu.VMEM)
    dma = pltpu.SemaphoreType.DMA
    rows = patch // (2 * groups)
    spots, everyone = groups * seq, 2 * groups * seq
    pairs = (
        [7, 3] + [seq - 1] * 2 + [spots - 1] * 2 + [seq - 1] * 2 + [5] * 2 + [everyone - 1] * 2 + [spots - 1] * 2
        + [seq - 1] * 2 + [2 * groups - 1] * 2 + [spots] * 2
    )
    attended, embed_grad = pl.pallas_call(
        functools.partial(fused, groups, seq),
        out_shape=(
            pltpu.VMEM((own_rows, width), b16),
            pltpu.VMEM((patch, model // 2), b16),
        ),
        in_specs=[pl.BlockSpec(memory_space=pltpu.HBM)] * 8,
        out_specs=(vmem, vmem),
        scratch_shapes=[
            pltpu.VMEM((4 * block, channels), b16),
            pltpu.VMEM((27 * lat_ch, channels), b16),
            pltpu.VMEM((1, lat_ch), f32),
            pltpu.VMEM((1, own_rows), jnp.int32),
            pltpu.VMEM((patch, model), b16),
            pltpu.VMEM((1, model), f32),
            pltpu.VMEM((own_rows, width), b16),
            pltpu.VMEM((3, depth, cols), b16),
            pltpu.VMEM((seq, 3 * patch // 2, pair), b16),
            pltpu.VMEM((seq - 1, 3 * patch // 2, pair), b16),
            pltpu.VMEM((spots, own_rows // 2, pair), b16),
            pltpu.VMEM((spots, own_rows // 2, pair), b16),
            pltpu.VMEM((seq, 1, own_rows), jnp.int32),
            pltpu.VMEM((3, block, patch), f32),
            pltpu.VMEM((3, block, patch), f32),
            pltpu.VMEM((5, block, patch), f32),
            pltpu.VMEM((block, patch), f32),
            pltpu.VMEM((everyone, block, patch), b16),
            pltpu.VMEM((spots, own_rows // 2, pair), b16),
            pltpu.VMEM((spots, own_rows // 2, pair), b16),
            pltpu.VMEM((tokens_all, tokens_all), b16),
            pltpu.VMEM((seq, 2 * patch, pair), b16),
            pltpu.VMEM((2 * groups, rows, depth), f32),
            pltpu.VMEM((2 * groups - 1, rows, depth), f32),
            pltpu.VMEM((rows, depth), b16),
            pltpu.VMEM((patch, model // 2), b16),
        ]
        + [dma((n,)) for n in pairs]
        + [dma],
        compiler_params=pltpu.CompilerParams(collective_id=0, has_side_effects=True),
    )(
        features.reshape(4 * block, channels),
        jnp.transpose(conv_weight, (0, 1, 2, 4, 3)).reshape(-1, channels),
        conv_bias.reshape(1, lat_ch),
        token_order.reshape(1, own_rows),
        embed_weight,
        norm_gain.reshape(1, model),
        jnp.transpose(qkv_weight, (1, 0, 2)),
        grad_out[0],
    )
    attended, embed_grad = pl.pallas_call(
        finish,
        out_shape=(
            jax.ShapeDtypeStruct((own_rows, width), b16),
            jax.ShapeDtypeStruct((patch, model // 2), f32),
        ),
        in_specs=[vmem, vmem],
        out_specs=(vmem, vmem),
        compiler_params=pltpu.CompilerParams(vmem_limit_bytes=4 << 20),
    )(attended, embed_grad)
    return attended[None], embed_grad


def fits(mesh, features, conv_weight, embed_weight, qkv_weight, token_order):
    groups, seq, heads = (mesh.shape[axis] for axis in ("grp", "seq", "head"))
    clips, frames, rows, columns, _ = features.shape
    width = qkv_weight.shape[2] // heads
    depth = qkv_weight.shape[0] // seq
    patch = embed_weight.shape[0]
    return (
        heads == 2
        and clips == groups
        and frames == seq
        and seq % 2 == 0
        and rows == 2 * heads
        and columns % 32 == 0
        and width == groups * seq * HEAD_DIM
        and (seq * HEAD_DIM) % 128 == 0
        and depth % 128 == 0
        and patch == 4 * conv_weight.shape[-1]
        and patch == HEAD_DIM
        and patch % (16 * groups) == 0
        and token_order.shape[0] == seq * columns
        and token_order.shape[0] % (32 * seq) == 0
        and token_order.shape[0] % 128 == 0
    )


def solution(mesh):
    placed = (
        P("grp", "seq", "head", None, None),
        P(),
        P(),
        P("seq"),
        P(),
        P(),
        P("seq", None, "head"),
        P("grp", "seq", "head"),
    )

    def run(features, conv_weight, conv_bias, token_order, embed_weight, norm_gain, qkv_weight, grad_out):
        body = per_device
        if fits(mesh, features, conv_weight, embed_weight, qkv_weight, token_order):
            body = functools.partial(fast_device, mesh.shape["grp"], mesh.shape["seq"])
        return jax.shard_map(
            body,
            mesh=mesh,
            in_specs=placed,
            out_specs=(P("grp", "seq", "head"), P(None, "head")),
            check_vma=False,
        )(features, conv_weight, conv_bias, token_order, embed_weight, norm_gain, qkv_weight, grad_out)

    return run
```
